32 devices in a mesh: tm: 4 (over y, x), sx: 2 (over core), sy: 4 (over z).
Axes of the slice: x: 2, y: 2, z: 4, core: 2. Of those that a mesh axis runs over, the one named last changes fastest.
Arguments:
- iterate: float32 [32, 512, 1024], P('tm', 'sx', 'sy'), may hold values from -6 to 6
- source: float32 [32, 512, 1024], P('tm', 'sx', 'sy'), may hold values from -6 to 6
- start_field: float32 [512, 1024], P('sx', 'sy'), may hold values from -6 to 6
- conduct: float32 [512, 1024], P('sx', 'sy'), may hold values from 0.2 to 5
Outputs:
- updated: float32 [32, 512, 1024], P('tm', 'sx', 'sy')
- coarse_residual: float32 [8, 512, 1024], P('tm', 'sx', 'sy')
The draws below stay inside these ranges and needn't reach their ends.
All inputs are finite; a program needn't handle non-finite values.
Results may differ from the reference program's by a relative error of at most 0.00002.
Values sent between devices are 32-bit elements; how exact they have to be, the bound alone decides.
A program may use at most 128 MiB of HBM per device.

```python
import math
import jax
import jax.numpy as jnp

FACTOR = 4
SWEEPS = 2
NT = 32
NX = 512
NY = 1024


def steps_of(own_key, shape, split, low, top_value):
    def one(position, blocks):
        heights = jax.random.uniform(jax.random.fold_in(jax.random.fold_in(own_key, 6), position), (blocks,), jnp.float32, low / len(split), top_value / len(split))
        return jnp.repeat(jnp.exp(heights), shape[position] // blocks).reshape((-1,) + (1,) * (len(shape) - position - 1))

    level = one(*split[0])
    for cut in split[1:]:
        level = level * one(*cut)
    return level


def bell_draw(stream_key, shape, scale, bound, split=(), dtype=jnp.bfloat16):
    result = jax.random.normal(stream_key, shape, jnp.float32) * scale
    if len(split) > 0:
        result = steps_of(stream_key, shape, split, -0.22, 0.18) * result
    return jnp.clip(result, min=-bound, max=bound).astype(dtype)


def setup_inputs(seed: int = 0) -> dict:
    key_of = jax.random.split(jax.random.key(seed), 5)
    iterate = bell_draw(key_of[0], (NT, NX, NY), 1.0, 6.0, ((0, 4), (1, 2), (2, 4)), jnp.float32)
    source = bell_draw(key_of[1], (NT, NX, NY), 1.0, 6.0, ((0, 4), (1, 2), (2, 4)), jnp.float32)
    start_field = bell_draw(key_of[2], (NX, NY), 1.0, 6.0, ((0, 2), (1, 4)), jnp.float32)
    conduct = jnp.clip(jnp.exp(math.log(5.0) - 3.218876 * jax.random.uniform(key_of[3], (NX, NY), jnp.float32) ** steps_of(key_of[3], (NX, NY), ((0, 2), (1, 4)), -0.2, 0.2)), 0.2, 5.0)
    return {"iterate": iterate, "source": source, "start_field": start_field, "conduct": conduct}


def neighbours(padded):
    total = padded[:, 2:, 1:-1] + padded[:, :-2, 1:-1]
    return total + padded[:, 1:-1, 2:] + padded[:, 1:-1, :-2]


def implicit_step(rhs, coeff):
    denom = 1.0 + 4.0 * coeff
    field = rhs
    for sweep in range(SWEEPS):
        padded = jnp.pad(field, ((0, 0), (1, 1), (1, 1)))
        field = (rhs + coeff * neighbours(padded)) / denom
    return field


def restrict(field):
    shape = field.shape
    blocks = field.reshape(shape[0], shape[1] // 2, 2, shape[2] // 2, 2)
    return 0.25 * jnp.sum(blocks, axis=(2, 4))


def prolong(field):
    return jnp.repeat(jnp.repeat(field, 2, axis=1), 2, axis=2)


def reference(iterate, source, start_field, conduct):
    count = NT // FACTOR
    state = iterate.reshape(count, FACTOR, NX, NY)
    forcing = source.reshape(count, FACTOR, NX, NY)

    def relax_fine(state):
        field = jnp.concatenate([start_field[None], state[:-1, FACTOR - 1]], axis=0)
        columns = []
        for place in range(FACTOR - 1):
            field = implicit_step(field + forcing[:, place], conduct)
            columns.append(field)
        columns.append(state[:, FACTOR - 1])
        return jnp.stack(columns, axis=1)

    def relax_coarse(state):
        point = implicit_step(state[:, FACTOR - 2] + forcing[:, FACTOR - 1], conduct)
        return state.at[:, FACTOR - 1].set(point)

    state = relax_fine(state)
    state = relax_coarse(state)
    state = relax_fine(state)
    resid = implicit_step(state[:, FACTOR - 2] + forcing[:, FACTOR - 1], conduct) - state[:, FACTOR - 1]
    coarse_rhs = restrict(resid)
    coarse_coeff = restrict(conduct[None])[0]
    error = jnp.zeros((1, NX // 2, NY // 2), jnp.float32)
    errors = []
    for level in range(count):
        error = implicit_step(error, coarse_coeff) + coarse_rhs[level][None]
        errors.append(error[0])
    correction = prolong(jnp.stack(errors, axis=0))
    state = state.at[:, FACTOR - 1].add(correction)
    state = relax_fine(state)
    return state.reshape(NT, NX, NY), resid
```

```python
import functools
import jax
import jax.numpy as jnp
from jax import lax
from jax.experimental import pallas as pl
from jax.experimental.pallas import tpu as pltpu
from jax.sharding import PartitionSpec as P

FACTOR = 4
SWEEPS = 2
LANES = 128
PAD = 8
STRIP = 32
MESH = pl.DeviceIdType.MESH


def round_up(value, unit):
    return -(-value // unit) * unit


def when_all(*conds):
    total = conds[0]
    for cond in conds[1:]:
        total = jnp.logical_and(total, cond)
    return pl.when(total)


def kernel(
    sizes, rows, cols, count,
    iterate_ref, source_ref, start_ref, conduct_ref,
    out_ref, resid_ref,
    fields, inv, gain, rhs, half, points,
    pack_right, pack_left, from_left, from_right,
    rc, errors, cinv, cgain, chalf,
    cpack_right, cpack_left, cfrom_left, cfrom_right,
    folded,
    local_sems, up_sems, side_sems, time_sems, rc_send, rc_recv, out_sems,
):
    nt, nx, ny = sizes
    t, x, y = lax.axis_index("tm"), lax.axis_index("sx"), lax.axis_index("sy")
    f32 = jnp.float32
    out_v, resid_v = out_ref, resid_ref
    halo = 2 * SWEEPS * FACTOR
    planes = cols // LANES
    top = PAD + halo
    ext = rows + 2 * halo
    levels = nt * count
    crows, cplanes = rows // 2, cols // 2 // LANES
    chalo = (rc.shape[2] - 2 * PAD - crows) // 2
    ctop = PAD + chalo
    cext = crows + 2 * chalo
    per_interval = FACTOR + 1
    n_first = 1 + per_interval * (count - 1)

    def base_of(k):
        return 1 + per_interval * (count - 1 - k) - (k == 0)

    def start_of(k):
        return base_of(k) if k > 0 else n_first + FACTOR

    def zero_rows(ref, start, size):
        ref[..., pl.ds(start, size), :] = jnp.zeros(ref.shape[:-2] + (size, LANES), f32)

    def zero_halos(i, carry):
        for p in range(planes):
            fields[i, p, pl.ds(PAD, halo), :] = jnp.zeros((halo, LANES), f32)
            fields[i, p, pl.ds(top + rows, halo), :] = jnp.zeros((halo, LANES), f32)
        return carry

    lax.fori_loop(0, fields.shape[0], zero_halos, 0)

    def zero_leading(ref):
        n = ref.shape[-2]

        def body(i, carry):
            ref[i] = jnp.zeros(ref.shape[1:], f32)
            return carry

        lax.fori_loop(0, ref.shape[0], body, 0)

    for ref in (from_left, from_right, cfrom_left, cfrom_right, rc, folded):
        zero_leading(ref)
    loads = []

    def load(src, field, sem):
        for p in range(planes):
            copy = pltpu.make_async_copy(
                src.at[:, pl.ds(p * LANES, LANES)],
                fields.at[field, p, pl.ds(top, rows), :],
                local_sems.at[sem + p],
            )
            copy.start()
            loads.append(copy)

    sem = 0
    load(conduct_ref, 0, sem)
    sem += planes
    for k in range(count - 1, -1, -1):
        if k > 0:
            load(iterate_ref.at[k * FACTOR - 1], start_of(k), sem)
            sem += planes
        for j in range(FACTOR):
            load(source_ref.at[k * FACTOR + j], base_of(k) + 1 + j, sem)
            sem += planes
    first_loads = len(loads) - planes * FACTOR
    opening = [
        pltpu.make_async_copy(
            start_ref.at[:, pl.ds(p * LANES, LANES)],
            fields.at[start_of(0), p, pl.ds(top, rows), :],
            local_sems.at[sem + p],
        )
        for p in range(planes)
    ]

    @pl.when(t == 0)
    def _():
        for copy in opening:
            copy.start()

    barrier = pltpu.get_barrier_semaphore()
    has_up, has_down = x > 0, x < nx - 1
    has_left, has_right = y > 0, y < ny - 1
    has_prev, has_next = t > 0, t < nt - 1
    arrivals = jnp.int32(nt - 1)
    for cond, target in (
        (has_up, {"sx": x - 1}), (has_down, {"sx": x + 1}),
        (has_left, {"sy": y - 1}), (has_right, {"sy": y + 1}),
    ):
        arrivals += jnp.where(cond, 1, 0)

        @pl.when(cond)
        def _(target=target):
            pl.semaphore_signal(barrier, inc=1, device_id=target, device_id_type=MESH)

    for other in range(nt):
        @pl.when(t != other)
        def _(other=other):
            pl.semaphore_signal(barrier, inc=1, device_id={"tm": other}, device_id_type=MESH)

    pl.semaphore_wait(barrier, arrivals)

    def remote(src, dst, sems, number, target):
        return pltpu.make_async_remote_copy(
            src_ref=src, dst_ref=dst, send_sem=sems.at[0, number], recv_sem=sems.at[1, number],
            device_id=target, device_id_type=MESH,
        )

    old = [
        remote(
            iterate_ref.at[count * FACTOR - 1, :, pl.ds(p * LANES, LANES)],
            fields.at[start_of(0), p, pl.ds(top, rows), :],
            time_sems, p, {"tm": t + 1},
        )
        for p in range(planes)
    ]

    @pl.when(has_next)
    def _():
        for copy in old:
            copy.start()

    lane = lax.broadcasted_iota(jnp.int32, (8, LANES), 1)

    def row_exchange(ref, lead, width, own_top, own_rows, depth, sems, number):
        def part(start):
            return ref.at[lead, pl.ds(0, width), pl.ds(start, depth), :]

        down = remote(part(own_top + own_rows - depth), part(own_top - depth), sems, number, {"sx": x + 1})
        up = remote(part(own_top), part(own_top + own_rows), sems, number + 1, {"sx": x - 1})

        @pl.when(has_down)
        def _():
            down.start()

        @pl.when(has_up)
        def _():
            up.start()

        @pl.when(has_up)
        def _():
            down.wait_recv()

        @pl.when(has_down)
        def _():
            up.wait_recv()

        @pl.when(has_down)
        def _():
            down.wait_send()

        @pl.when(has_up)
        def _():
            up.wait_send()

    def side_exchange(ref, first, slots, width, depth, length, right, left, in_left, in_right, tile0, sems, number):
        per_tile = LANES // depth
        tiles = -(-slots // per_tile)
        chunk = 32
        for tile in range(tiles):
            members = range(tile * per_tile, min(slots, (tile + 1) * per_tile))
            wide = lax.broadcasted_iota(jnp.int32, (chunk, LANES), 1)

            def pack(i, carry, members=members, tile=tile):
                at = pl.ds(PAD + i * chunk, chunk)
                to_right = to_left = jnp.zeros((chunk, LANES), f32)
                for place, slot in enumerate(members):
                    here = jnp.logical_and(wide >= place * depth, wide < (place + 1) * depth)
                    last, head = ref[first + slot, width - 1, at, :], ref[first + slot, 0, at, :]
                    to_right = jnp.where(here, pltpu.roll(last, (place * depth + depth) % LANES, 1), to_right)
                    to_left = jnp.where(here, pltpu.roll(head, place * depth, 1), to_left)
                right[tile0 + tile, pl.ds(i * chunk, chunk), :] = to_right
                left[tile0 + tile, pl.ds(i * chunk, chunk), :] = to_left
                return carry

            lax.fori_loop(0, length // chunk, pack, 0)
        span = pl.ds(tile0, tiles)
        go_right = remote(right.at[span], in_left.at[span], sems, number, {"sy": y + 1})
        go_left = remote(left.at[span], in_right.at[span], sems, number + 1, {"sy": y - 1})

        @pl.when(has_right)
        def _():
            go_right.start()

        @pl.when(has_left)
        def _():
            go_left.start()

        def finish():
            @pl.when(has_left)
            def _():
                go_right.wait_recv()

            @pl.when(has_right)
            def _():
                go_left.wait_recv()

            for tile in range(tiles):
                members = range(tile * per_tile, min(slots, (tile + 1) * per_tile))
                wide = lax.broadcasted_iota(jnp.int32, (chunk, LANES), 1)

                def unpack(i, carry, members=members, tile=tile):
                    at = pl.ds(PAD + i * chunk, chunk)
                    came_right = in_right[tile0 + tile, pl.ds(i * chunk, chunk), :]
                    came_left = in_left[tile0 + tile, pl.ds(i * chunk, chunk), :]
                    for place, slot in enumerate(members):
                        on_right = pltpu.roll(came_right, (-place * depth) % LANES, 1)
                        on_left = pltpu.roll(came_left, (LANES - depth - place * depth) % LANES, 1)
                        ref[first + slot, width, at, :] = jnp.where(
                            wide < depth, on_right, jnp.where(wide >= LANES - depth, on_left, 0.0)
                        )
                    return carry

                lax.fori_loop(0, length // chunk, unpack, 0)

            @pl.when(has_right)
            def _():
                go_right.wait_send()

            @pl.when(has_left)
            def _():
                go_left.wait_send()

        return finish

    groups = LANES // (2 * halo)
    seg = ext // groups

    def fold(plane, dst):
        wide = lax.broadcasted_iota(jnp.int32, (seg, LANES), 1)
        total = jnp.zeros((seg, LANES), f32)
        for g in range(groups):
            part = pltpu.roll(plane[pl.ds(PAD + g * seg, seg), :], (halo + 2 * halo * g) % LANES, 1)
            total = jnp.where(wide // (2 * halo) == g, part, total)
        dst[...] = total

    def unfold(on_right, on_left, plane):
        wide = lax.broadcasted_iota(jnp.int32, (seg, LANES), 1)
        for g in range(groups):
            back = (-(halo + 2 * halo * g)) % LANES
            plane[pl.ds(PAD + g * seg, seg), :] = jnp.where(
                wide < halo, pltpu.roll(on_right[...], back, 1),
                jnp.where(wide >= LANES - halo, pltpu.roll(on_left[...], back, 1), 0.0),
            )

    def strips(length, body, lead=0):
        for start in range(0, length, STRIP):
            body(lead + start, min(STRIP, length - start))

    def total_of(ref, width, at, size):
        wide = lax.broadcasted_iota(jnp.int32, (size, LANES), 1)
        ahead, behind = [], []
        for p in range(width):
            own = ref[p, pl.ds(at, size), :]
            behind.append(pltpu.roll(own, 1, 1))
            ahead.append(pltpu.roll(own, LANES - 1, 1))
        result = []
        for p in range(width):
            vert = ref[p, pl.ds(at + 1, size), :] + ref[p, pl.ds(at - 1, size), :]
            nxt = jnp.where(wide == LANES - 1, ahead[(p + 1) % width], ahead[p])
            prv = jnp.where(wide == 0, behind[(p - 1) % width], behind[p])
            result.append(vert + (nxt + prv))
        return result

    def sweep(src, b, ivs, gs, width, length, emit, lead):
        def body(offset, size):
            at = PAD + offset
            sums = total_of(src, width, at, size)
            for p in range(width):
                rows_at = pl.ds(at, size)
                emit(p, offset, size, b[p, rows_at, :] * ivs[p, rows_at, :] + gs[p, rows_at, :] * sums[p])

        strips(length, body, lead)

    def phi(b, emit, ivs=inv, gs=gain, mid=half, width=planes + 1, length=ext, lead=0):
        def keep(p, offset, size, value):
            mid[p, pl.ds(PAD + offset, size), :] = value

        sweep(b, b, ivs, gs, width, length, keep, lead)
        sweep(mid, b, ivs, gs, width, length, emit, lead)

    def fill(value):
        def body(offset, size):
            at = pl.ds(PAD + offset, size)
            for p in range(planes + 1):
                rhs[p, at, :] = value(p, at)

        strips(ext, body)

    def first_pass(k):
        base = base_of(k)
        fill(lambda p, at: fields[start_of(k), p, at, :] + fields[base + 1, p, at, :])

        def one(j, carry):
            def emit(p, offset, size, value):
                at = pl.ds(PAD + offset, size)
                rhs[p, at, :] = value + fields[base + 2 + j, p, at, :]

            phi(rhs, emit)
            return carry

        lax.fori_loop(0, FACTOR - 1, one, 0)

        def last(p, offset, size, value):
            points[k + 1, p, pl.ds(PAD + offset, size), :] = value

        phi(rhs, last)

    def coefficients(src, ivs, gs, width, length):
        def body(offset, size):
            at = pl.ds(PAD + offset, size)
            for p in range(width):
                c = src[p, at, :]
                one = 1.0 / (1.0 + 4.0 * c)
                ivs[p, at, :] = one
                gs[p, at, :] = c * one

        strips(length, body)

    lane_in = lax.broadcasted_iota(jnp.int32, (LANES, LANES), 0)
    lane_out = lax.broadcasted_iota(jnp.int32, (LANES, LANES), 1)

    def dot(a, b):
        return jnp.dot(a, b, precision=lax.Precision.HIGHEST, preferred_element_type=f32)

    def restrict(ref, own_top, store):
        pairs = []
        for p in range(planes):
            pairs.append(ref[p, pl.ds(own_top, crows, stride=2), :] + ref[p, pl.ds(own_top + 1, crows, stride=2), :])
        for q in range(cplanes):
            value = jnp.zeros((crows, LANES), f32)
            for side in range(2):
                pick = jnp.where(lane_in // 2 + side * (LANES // 2) == lane_out, 0.25, 0.0)
                value += dot(pairs[2 * q + side], pick)
            store(q, value)

    for copy in loads[:first_loads]:
        copy.wait()

    def keep_coarse(q, value):
        rc[0, q, pl.ds(ctop, crows), :] = value

    first_tiles = -(-n_first // (LANES // halo))
    row_exchange(fields, pl.ds(0, n_first), planes, top, rows, halo, up_sems, 0)
    finish = side_exchange(
        fields, 0, n_first, planes, halo, ext, pack_right, pack_left, from_left, from_right, 0, side_sems, 0
    )
    for copy in loads[first_loads:]:
        copy.wait()
    row_exchange(fields, pl.ds(n_first, FACTOR), planes, top, rows, halo, up_sems, 2)
    finish_sources = side_exchange(
        fields, n_first, FACTOR, planes, halo, ext,
        pack_right, pack_left, from_left, from_right, first_tiles, side_sems, 2,
    )
    for ref in (rhs, half, chalf):
        zero_rows(ref, 0, PAD)
        zero_rows(ref, ref.shape[-2] - PAD, PAD)
    zero_leading(errors)
    for start in (PAD, top + rows + halo // 2):
        points[0, :, pl.ds(start, halo // 2), :] = jnp.zeros((planes + 1, halo // 2, LANES), f32)
    restrict(fields.at[0], top, keep_coarse)
    finish()
    coefficients(fields.at[0], inv, gain, planes + 1, ext)
    near = pl.ds(top - halo // 2, rows + halo)
    for k in range(count - 1, 0, -1):
        first_pass(k)
        if k == count - 1:
            fold(points.at[count, planes], folded.at[0])
            sent = [
                remote(points.at[count, pl.ds(0, planes), near, :], points.at[0, pl.ds(0, planes), near, :], time_sems, planes, {"tm": t + 1}),
                remote(folded.at[0], folded.at[1], time_sems, planes + 1, {"tm": t + 1}),
            ]

            @pl.when(has_next)
            def _():
                for copy in sent:
                    copy.start()

    @pl.when(t == 0)
    def _():
        for copy in opening:
            copy.wait()

    @pl.when(has_prev)
    def _():
        for copy in old:
            copy.wait_recv()

    last_field = n_first + FACTOR
    row_exchange(fields, pl.ds(last_field, 1), planes, top, rows, halo, up_sems, 6)
    fold(fields.at[last_field, planes - 1], folded.at[2])
    fold(fields.at[last_field, 0], folded.at[3])
    go_right = remote(folded.at[2], folded.at[4], side_sems, 6, {"sy": y + 1})
    go_left = remote(folded.at[3], folded.at[5], side_sems, 7, {"sy": y - 1})

    @pl.when(has_right)
    def _():
        go_right.start()

    @pl.when(has_left)
    def _():
        go_left.start()

    finish_sources()

    @pl.when(has_left)
    def _():
        go_right.wait_recv()

    @pl.when(has_right)
    def _():
        go_left.wait_recv()

    unfold(folded.at[5], folded.at[4], fields.at[last_field, planes])

    @pl.when(has_right)
    def _():
        go_right.wait_send()

    @pl.when(has_left)
    def _():
        go_left.wait_send()

    first_pass(0)

    trim = dict(length=rows + halo, lead=halo // 2)
    stores = []

    def put(src, dst, number):
        pass

    def level_of(block, k):
        return rc.at[pl.ds(1 + block * count + k, 1), pl.ds(0, cplanes), pl.ds(ctop, crows), :]

    def level_copy(block, k, other):
        return pltpu.make_async_remote_copy(
            src_ref=level_of(block, k), dst_ref=level_of(block, k),
            send_sem=rc_send.at[other, k], recv_sem=rc_recv.at[block, k],
            device_id={"tm": other}, device_id_type=MESH,
        )

    def residual(k):
        fill(lambda p, at: points[k, p, at, :] - fields[start_of(k), p, at, :])

        def one(j, carry):
            def emit(p, offset, size, value):
                rhs[p, pl.ds(PAD + offset, size), :] = value

            phi(rhs, emit, **trim)
            return carry

        lax.fori_loop(0, FACTOR, one, 0)

        def store(q, value):
            rc[1 + t * count + k, q, pl.ds(ctop, crows), :] = value

        restrict(rhs, top, store)
        for other in range(1, nt):
            copy = level_copy(t, k, other)

            @pl.when(t < other)
            def _(copy=copy):
                copy.start()

        for p in range(planes):
            resid_v[k, :, pl.ds(p * LANES, LANES)] = rhs[p, pl.ds(top, rows), :]
        put(resid_v.at[k], resid_ref.at[k], count * FACTOR + k)

    for k in range(count - 1, 0, -1):
        residual(k)

    @pl.when(t == 0)
    def _():
        for p in range(planes + 1):
            points[0, p, near, :] = fields[start_of(0), p, near, :]

    @pl.when(has_prev)
    def _():
        for copy in sent:
            copy.wait_recv()
        unfold(folded.at[1], folded.at[1], points.at[0, planes])

    residual(0)

    for other in range(nt - 1):
        @pl.when(t > other)
        def _(other=other):
            for k in range(count):
                level_copy(other, k, other).wait_recv()

    for other in range(1, nt):
        @pl.when(t < other)
        def _(other=other):
            for k in range(count):
                level_copy(t, k, other).wait_send()

    row_exchange(rc, pl.ds(0, levels), cplanes, ctop, crows, chalo, up_sems, 4)
    finish = side_exchange(
        rc, 0, levels, cplanes, chalo, cext,
        cpack_right, cpack_left, cfrom_left, cfrom_right, 0, side_sems, 4,
    )
    finish()
    coefficients(rc.at[0], cinv, cgain, cplanes + 1, cext)

    def level(n, carry):
        def emit(p, offset, size, value):
            at = pl.ds(PAD + offset, size)
            errors[n + 1, p, at, :] = value + rc[n + 1, p, at, :]

        phi(errors.at[n], emit, cinv, cgain, chalf, cplanes + 1, cext)
        return carry

    lax.fori_loop(0, levels, level, 0)

    picks = []
    for p in range(planes):
        picks.append(jnp.where(lane_in == lane_out // 2 + (p % 2) * (LANES // 2), 1.0, 0.0))
    rim = jnp.where(lane_out < LANES // 2, lane_out // 2, LANES // 2 + lane_out // 2)
    picks.append(jnp.where(lane_in == rim, 1.0, 0.0))
    span = ext // 2
    shift = ctop - halo // 2

    def correct(k):
        for p in range(planes + 1):
            plane = errors[t * count + k, cplanes if p == planes else p // 2, pl.ds(shift, span), :]
            wide = dot(plane, picks[p])
            for odd in range(2):
                half[p, pl.ds(PAD + odd, span, stride=2), :] = wide

        def body(offset, size):
            at = pl.ds(PAD + offset, size)
            for p in range(planes + 1):
                points[k, p, at, :] = points[k, p, at, :] + half[p, at, :]

        strips(rows + halo, body, halo // 2)

    @pl.when(has_next)
    def _():
        for copy in sent + old:
            copy.wait_send()

    for k in range(count + 1):
        correct(k)
        if k > 0:
            for p in range(planes):
                out_v[k * FACTOR - 1, :, pl.ds(p * LANES, LANES)] = points[k, p, pl.ds(top, rows), :]
            put(out_v.at[k * FACTOR - 1], out_ref.at[k * FACTOR - 1], k * FACTOR - 1)

    for k in range(count):
        base = base_of(k)
        fill(lambda p, at: points[k, p, at, :] + fields[base + 1, p, at, :])
        for j in range(FACTOR - 1):
            def emit(p, offset, size, value, j=j):
                at = pl.ds(PAD + offset, size)
                if j < FACTOR - 2:
                    rhs[p, at, :] = value + fields[base + 2 + j, p, at, :]
                low, high = max(offset, halo), min(offset + size, halo + rows)
                if p < planes and low < high:
                    own = value[low - offset : high - offset]
                    out_v[k * FACTOR + j, pl.ds(low - halo, high - low), pl.ds(p * LANES, LANES)] = own

            phi(rhs, emit, **trim)
            put(out_v.at[k * FACTOR + j], out_ref.at[k * FACTOR + j], k * FACTOR + j)

    for copy in stores:
        copy.wait()


def solution(mesh):
    sizes = tuple(mesh.shape[name] for name in ("tm", "sx", "sy"))

    def shards(iterate, source, start_field, conduct):
        steps, rows, cols = iterate.shape
        count = steps // FACTOR
        levels = sizes[0] * count
        halo = 2 * SWEEPS * FACTOR
        planes, cplanes = cols // LANES, cols // 2 // LANES
        tall = rows + 2 * halo + 2 * PAD
        chalo = round_up(SWEEPS * levels, 16)
        ctall = rows // 2 + 2 * chalo + 2 * PAD
        n_fields = 1 + (FACTOR + 1) * count
        per_tile = LANES // halo
        tiles = -(-(n_fields - FACTOR - 1) // per_tile) + 1
        ctiles = -(-levels // (LANES // chalo))
        f32 = jnp.float32
        field = pltpu.VMEM((planes + 1, tall, LANES), f32)
        packed = pltpu.VMEM((tiles, rows + 2 * halo, LANES), f32)
        cfield = pltpu.VMEM((cplanes + 1, ctall, LANES), f32)
        cpacked = pltpu.VMEM((ctiles, rows // 2 + 2 * chalo, LANES), f32)
        n_loads = planes * (n_fields + 1)
        dma = pltpu.SemaphoreType.DMA
        res = pl.pallas_call(
            functools.partial(kernel, sizes, rows, cols, count),
            out_shape=(
                pltpu.VMEM((steps, rows, cols), f32),
                pltpu.VMEM((count, rows, cols), f32),
            ),
            in_specs=[pl.BlockSpec(memory_space=pltpu.MemorySpace.HBM)] * 4,
            out_specs=[pl.BlockSpec(memory_space=pltpu.MemorySpace.VMEM)] * 2,
            scratch_shapes=[
                pltpu.VMEM((n_fields, planes + 1, tall, LANES), f32),
                field, field, field, field,
                pltpu.VMEM((count + 1, planes + 1, tall, LANES), f32),
                packed, packed, packed, packed,
                pltpu.VMEM((levels + 1, cplanes + 1, ctall, LANES), f32),
                pltpu.VMEM((levels + 1, cplanes + 1, ctall, LANES), f32),
                cfield, cfield, cfield,
                cpacked, cpacked, cpacked, cpacked,
                pltpu.VMEM((6, (rows + 2 * halo) // (LANES // (2 * halo)), LANES), f32),
                dma((n_loads,)), dma((2, 8)), dma((2, 8)), dma((2, planes + 2)),
                dma((sizes[0], count)), dma((sizes[0], count)), dma((steps + count,)),
            ],
            compiler_params=pltpu.CompilerParams(
                collective_id=0, has_side_effects=True, vmem_limit_bytes=48 * 1024 * 1024
            ),
        )(*[pltpu.with_memory_space_constraint(z, pltpu.MemorySpace.HBM) for z in (iterate, source, start_field, conduct)])

        def put(a, b, oa, ob, sems):
            n = a.shape[0]
            cs = [pltpu.make_async_copy(a.at[i], oa.at[i], sems.at[i]) for i in range(n)]
            cs += [pltpu.make_async_copy(b.at[i], ob.at[i], sems.at[n + i]) for i in range(b.shape[0])]
            for c in cs:
                c.start()
            for c in cs:
                c.wait()

        return pl.pallas_call(
            put,
            out_shape=(jax.ShapeDtypeStruct((steps, rows, cols), f32), jax.ShapeDtypeStruct((count, rows, cols), f32)),
            in_specs=[pl.BlockSpec(memory_space=pltpu.MemorySpace.VMEM)] * 2,
            out_specs=[pl.BlockSpec(memory_space=pltpu.MemorySpace.HBM)] * 2,
            scratch_shapes=[dma((steps + count,))],
        )(*[pltpu.with_memory_space_constraint(z, pltpu.MemorySpace.VMEM) for z in res])

    in_specs = (P("tm", "sx", "sy"), P("tm", "sx", "sy"), P("sx", "sy"), P("sx", "sy"))
    out_specs = (P("tm", "sx", "sy"), P("tm", "sx", "sy"))
    return jax.shard_map(shards, mesh=mesh, in_specs=in_specs, out_specs=out_specs, check_vma=False)
```
